16 devices in a mesh: dp: 2 (over z), emb: 8 (over y, x, core).
Axes of the slice: x: 2, y: 2, z: 2, core: 2. Of those that a mesh axis runs over, the one named last changes fastest.
Arguments:
- tok_ids: int32 [16384], P(('dp', 'emb'))
- resid_in: bfloat16 [16384, 768], P(('dp', 'emb'))
- cot_out: bfloat16 [16384, 768], P(('dp', 'emb'))
- tables: bfloat16 [6, 50304, 768], P(None, 'emb')
- w_up: bfloat16 [6, 768, 3072], replicated
- w_down: bfloat16 [6, 3072, 768], replicated
- w_gate: bfloat16 [6, 768, 768], replicated
- w_proj: bfloat16 [6, 768, 768], replicated
Outputs:
- output 1: bfloat16 [16384, 768], P(('dp', 'emb'))
- output 2: float32 [6, 50304, 768], P(None, 'emb')
All inputs are finite; a program needn't handle non-finite values.
Results may differ from the reference program's by a relative error of at most 0.0151457.
Values are sent between devices in bfloat16 or wider.
A program may use at most 1 GiB of HBM per device.

```python
import jax
import jax.numpy as jnp
from jax import lax

TOKENS_DEV = 1024
LAYERS = 6
D_MODEL = 768
FFN_DIM = 3072
EMB_DIM = 768
VOCAB_SIZE = 50304
NUM_DP = 2
NUM_EMB = 8
CAP_ROWS = 256

N_TOKENS = TOKENS_DEV * NUM_DP * NUM_EMB
RANGE_ROWS = VOCAB_SIZE // NUM_EMB
HOT_SET = min(16, RANGE_ROWS)
NORM_EPS = 1e-6


def draw_ids(id_key):
    key_list = jax.random.split(id_key, 9)
    n_dev = NUM_DP * NUM_EMB
    draw_shape = (n_dev, TOKENS_DEV)
    tok_pos = jnp.arange(TOKENS_DEV, dtype=jnp.int32)[None, :]
    hot_top = jax.random.randint(key_list[0], (n_dev, 1), 1, NUM_EMB + 1)
    hot_owner = jax.random.randint(key_list[1], (n_dev, 1), 0, hot_top)
    shift_by = jax.random.randint(key_list[2], (n_dev, 1), 0, NUM_EMB - 1)
    spread = (hot_owner + 1 + (tok_pos - CAP_ROWS + shift_by) % (NUM_EMB - 1)) % NUM_EMB
    owner_seq = jnp.where(tok_pos < CAP_ROWS, hot_owner, spread)
    scores = jax.random.randint(key_list[3], draw_shape, 0, TOKENS_DEV) * TOKENS_DEV + tok_pos
    perm_order = jnp.argsort(scores, axis=1)
    owner_ids = jnp.take_along_axis(owner_seq, perm_order, axis=1)
    is_hot = jax.random.randint(key_list[4], draw_shape, 0, 4) == 0
    hot_off = jax.random.randint(key_list[5], draw_shape, 0, HOT_SET)
    span_a = jax.random.randint(key_list[6], draw_shape, 1, RANGE_ROWS + 1)
    span_b = jax.random.randint(key_list[7], draw_shape, 1, span_a + 1)
    tail_off = jax.random.randint(key_list[8], draw_shape, 0, span_b)
    offset = jnp.where(is_hot, hot_off, tail_off)
    return (owner_ids * RANGE_ROWS + offset).reshape(-1).astype(jnp.int32)


def setup_inputs(seed: int = 0) -> dict:
    root_key = jax.random.key(seed)
    key_list = jax.random.split(root_key, 8)
    tok_ids = draw_ids(key_list[0])
    resid_in = jax.random.normal(key_list[1], (N_TOKENS, D_MODEL), jnp.float32).astype(jnp.bfloat16)
    cot_out = jax.random.normal(key_list[2], (N_TOKENS, D_MODEL), jnp.float32).astype(jnp.bfloat16)
    tables = (0.5 * jax.random.normal(key_list[3], (LAYERS, VOCAB_SIZE, EMB_DIM), jnp.float32)).astype(jnp.bfloat16)
    w_up = (jax.random.normal(key_list[4], (LAYERS, D_MODEL, FFN_DIM), jnp.float32) * D_MODEL ** -0.5).astype(jnp.bfloat16)
    w_down = (jax.random.normal(key_list[5], (LAYERS, FFN_DIM, D_MODEL), jnp.float32) * (0.5 * FFN_DIM ** -0.5)).astype(jnp.bfloat16)
    w_gate = (jax.random.normal(key_list[6], (LAYERS, D_MODEL, EMB_DIM), jnp.float32) * D_MODEL ** -0.5).astype(jnp.bfloat16)
    w_proj = (jax.random.normal(key_list[7], (LAYERS, EMB_DIM, D_MODEL), jnp.float32) * EMB_DIM ** -0.5).astype(jnp.bfloat16)
    return {'tok_ids': tok_ids, 'resid_in': resid_in, 'cot_out': cot_out, 'tables': tables, 'w_up': w_up, 'w_down': w_down, 'w_gate': w_gate, 'w_proj': w_proj}


def rms_norm(x_f32):
    return x_f32 * lax.rsqrt(jnp.mean(x_f32 * x_f32, axis=-1, keepdims=True) + NORM_EPS)


def layer_forward(resid_cur, fetched, w_up_l, w_down_l, w_gate_l, w_proj_l):
    x_f32 = resid_cur.astype(jnp.float32)
    normed = rms_norm(x_f32).astype(jnp.bfloat16)
    hidden = jax.nn.gelu(jnp.dot(normed, w_up_l, preferred_element_type=jnp.float32)).astype(jnp.bfloat16)
    mlp_out = jnp.dot(hidden, w_down_l, preferred_element_type=jnp.float32)
    gate_act = jax.nn.gelu(jnp.dot(normed, w_gate_l, preferred_element_type=jnp.float32))
    mixed_in = (gate_act * fetched).astype(jnp.bfloat16)
    proj_out = jnp.dot(mixed_in, w_proj_l, preferred_element_type=jnp.float32)
    return (x_f32 + mlp_out + proj_out).astype(jnp.bfloat16)


def reference(tok_ids, resid_in, cot_out, tables, w_up, w_down, w_gate, w_proj):
    def fwd_step(resid_cur, layer_params):
        table_l, w_up_l, w_down_l, w_gate_l, w_proj_l = layer_params
        fetched = jnp.take(table_l, tok_ids, axis=0).astype(jnp.float32)
        resid_next = layer_forward(resid_cur, fetched, w_up_l, w_down_l, w_gate_l, w_proj_l)
        return resid_next, resid_cur

    resid_out, resid_saved = lax.scan(fwd_step, resid_in, (tables, w_up, w_down, w_gate, w_proj))

    def bwd_step(cot_next, layer_params):
        resid_cur, table_l, w_up_l, w_down_l, w_gate_l, w_proj_l = layer_params
        fetched = jnp.take(table_l, tok_ids, axis=0).astype(jnp.float32)

        def local_layer(resid_arg, fetched_arg):
            return layer_forward(resid_arg, fetched_arg, w_up_l, w_down_l, w_gate_l, w_proj_l)

        pullback = jax.vjp(local_layer, resid_cur, fetched)[1]
        cot_cur, d_fetched = pullback(cot_next)
        d_table = jax.ops.segment_sum(d_fetched, tok_ids, num_segments=VOCAB_SIZE)
        return cot_cur, d_table

    cot_first, d_tables = lax.scan(bwd_step, cot_out, (resid_saved, tables, w_up, w_down, w_gate, w_proj), reverse=True)
    return resid_out, d_tables
```

```python
import jax
import jax.numpy as jnp
from jax import lax
from jax.experimental import pallas as pl
from jax.experimental.pallas import tpu as pltpu
from jax.sharding import PartitionSpec as P


NORM_EPS = 1e-6
GELU_C = 0.7978845608028654
GELU_A = 0.044715
TILE = 256
BLK = 256
GBLK = 512
FCH = 768
F32 = jnp.float32
BF16 = jnp.bfloat16
SENT = 8191


def gelu_and_grad(x):
    x2 = x * x
    t = jnp.tanh(x * (GELU_C + (GELU_C * GELU_A) * x2))
    h = 0.5 + 0.5 * t
    grad = h + (0.5 * x) * (1.0 - t * t) * (GELU_C + (3.0 * GELU_C * GELU_A) * x2)
    return x * h, grad


def nn(a, b):
    return lax.dot_general(a, b, (((1,), (0,)), ((), ())), preferred_element_type=F32)


def nt(a, b):
    return lax.dot_general(a, b, (((1,), (1,)), ((), ())), preferred_element_type=F32)


def norm_stats(xf):
    return lax.rsqrt(jnp.mean(xf * xf, axis=-1, keepdims=True) + NORM_EPS)


def permute_kernel(n_ref, slot_ref, src_ref, out_ref, acc_ref):
    n_slots = src_ref.shape[0]

    @pl.when(pl.program_id(0) < n_ref[0])
    def _():
        slot = slot_ref[...]
        chunk = 512
        acc_ref[...] = jnp.zeros_like(acc_ref)
        for c in range(n_slots // chunk):
            cols = lax.broadcasted_iota(jnp.int32, (TILE, chunk), 1) + c * chunk
            sel = jnp.where(slot == cols, 1.0, 0.0).astype(BF16)
            acc_ref[...] += nn(sel, src_ref[c * chunk:(c + 1) * chunk, :])
        out_ref[...] = acc_ref[...].astype(BF16)


def permute(n_tiles, slot_col, src):
    n_slots, width = src.shape
    tile = lambda i, n: (jnp.minimum(i, n[0] - 1), 0)
    return pl.pallas_call(
        permute_kernel,
        grid_spec=pltpu.PrefetchScalarGridSpec(
            num_scalar_prefetch=1,
            grid=(n_slots // TILE,),
            in_specs=[
                pl.BlockSpec((TILE, 1), tile),
                pl.BlockSpec((n_slots, width), lambda i, n: (0, 0), pipeline_mode=pl.Buffered(1)),
            ],
            out_specs=pl.BlockSpec((TILE, width), tile),
            scratch_shapes=[pltpu.VMEM((TILE, width), F32)],
        ),
        out_shape=jax.ShapeDtypeStruct((n_slots, width), BF16),
        compiler_params=pltpu.CompilerParams(dimension_semantics=("arbitrary",)),
        name="permute",
    )(n_tiles, slot_col, src)


def gather_kernel(n_ref, lo_ref, hi_ref, ids_ref, table_ref, out_ref, acc_ref):
    range_rows = table_ref.shape[1]

    def tile_step(i, carry):
        rows = pl.ds(pl.multiple_of(i * TILE, TILE), TILE)
        ids = ids_ref[rows, :]

        def part(b):
            start = pl.multiple_of(jnp.minimum(b * GBLK, range_rows - GBLK), 16)
            cols = lax.broadcasted_iota(jnp.int32, (TILE, GBLK), 1) + start
            sel = jnp.where((ids == cols) & (cols >= b * GBLK), 1.0, 0.0).astype(BF16)
            return nn(sel, table_ref[0, pl.ds(start, GBLK), :])

        acc_ref[...] = part(lo_ref[i])

        def step(b, c):
            acc_ref[...] += part(b)
            return c

        lax.fori_loop(lo_ref[i] + 1, hi_ref[i] + 1, step, 0)
        out_ref[0, rows, :] = acc_ref[...].astype(BF16)
        return carry

    lax.fori_loop(0, n_ref[0], tile_step, 0)


def gather(n_tiles, lo, hi, ids_col, tables):
    n_layers, range_rows, e = tables.shape
    n_slots = ids_col.shape[0]
    return pl.pallas_call(
        gather_kernel,
        grid_spec=pltpu.PrefetchScalarGridSpec(
            num_scalar_prefetch=3,
            grid=(n_layers,),
            in_specs=[
                pl.BlockSpec((n_slots, 1), lambda l, *_: (0, 0)),
                pl.BlockSpec((1, range_rows, e), lambda l, *_: (l, 0, 0)),
            ],
            out_specs=pl.BlockSpec((1, n_slots, e), lambda l, *_: (l, 0, 0)),
            scratch_shapes=[pltpu.VMEM((TILE, e), F32)],
        ),
        out_shape=jax.ShapeDtypeStruct((n_layers, n_slots, e), BF16),
        compiler_params=pltpu.CompilerParams(dimension_semantics=("arbitrary",)),
        cost_estimate=pl.CostEstimate(flops=60_000_000_000, bytes_accessed=80_000_000, transcendentals=0),
        name="gather",
    )(n_tiles, lo, hi, ids_col, tables)


def weight_copies(hbm, bufs, sems, layer, slot):
    return [pltpu.make_async_copy(h.at[layer], v.at[slot], sems.at[slot, k]) for k, (h, v) in enumerate(zip(hbm, bufs))]


def next_weights(hbm, bufs, sems, step, n_steps, layer_of):
    slot = lax.rem(step, 2)

    @pl.when(step == 0)
    def _():
        for c in weight_copies(hbm, bufs, sems, layer_of(step), slot):
            c.start()

    for c in weight_copies(hbm, bufs, sems, layer_of(step), slot):
        c.wait()

    @pl.when(step + 1 < n_steps)
    def _():
        for c in weight_copies(hbm, bufs, sems, layer_of(step + 1), 1 - slot):
            c.start()


def weight_scratch(d, ffn, e):
    return [
        pltpu.VMEM((2, d, ffn), BF16),
        pltpu.VMEM((2, ffn, d), BF16),
        pltpu.VMEM((2, d, e), BF16),
        pltpu.VMEM((2, e, d), BF16),
        pltpu.SemaphoreType.DMA((2, 4)),
    ]


def fwd_kernel(n_ref, *refs):
    @pl.when(pl.program_id(1) < n_ref[0])
    def _():
        fwd_tile(*refs)


def fwd_tile(x0_ref, e_ref, w_up, w_down, w_gate, w_proj, xs_ref, g_ref, ge_ref, ug_ref, xl_ref,
             x_scr, m_scr, up_buf, down_buf, gate_buf, proj_buf, w_sems):
    l = pl.program_id(0)
    i = pl.program_id(1)
    n_layers = pl.num_programs(0)
    slot = lax.rem(l, 2)
    rows = pl.ds(pl.multiple_of(i * TILE, TILE), TILE)

    @pl.when(i == 0)
    def _():
        next_weights((w_up, w_down, w_gate, w_proj), (up_buf, down_buf, gate_buf, proj_buf), w_sems, l, n_layers, lambda q: q)

    @pl.when(l == 0)
    def _():
        x_scr[rows, :] = x0_ref[...]

    x = x_scr[rows, :]
    xs_ref[0] = x
    xf = x.astype(F32)
    u = (xf * norm_stats(xf)).astype(BF16)
    gate, gate_grad = gelu_and_grad(nn(u, gate_buf[slot]))
    emb = e_ref[0].astype(F32)
    g_ref[0] = gate
    ge_ref[0] = gate_grad * emb
    m_scr[...] = xf + nn((gate * emb).astype(BF16), proj_buf[slot])
    ffn = up_buf.shape[2]
    for c in range(ffn // FCH):
        cs = slice(c * FCH, (c + 1) * FCH)
        hid, hid_grad = gelu_and_grad(nn(u, up_buf[slot, :, cs]))
        ug_ref[0, :, cs] = hid_grad
        m_scr[...] += nn(hid.astype(BF16), down_buf[slot, cs, :])
    x_next = m_scr[...].astype(BF16)
    x_scr[rows, :] = x_next

    @pl.when(l == n_layers - 1)
    def _():
        xl_ref[...] = x_next


def forward(n_tiles, x0, es, w_up, w_down, w_gate, w_proj):
    n_layers, n_slots, e = es.shape
    d = x0.shape[1]
    ffn = w_up.shape[2]
    tile = lambda l, i, n: (l, jnp.minimum(i, n[0] - 1), 0)
    only = lambda which: (lambda l, i, n: (jnp.where(l == which, jnp.minimum(i, n[0] - 1), 0), 0))
    return pl.pallas_call(
        fwd_kernel,
        grid_spec=pltpu.PrefetchScalarGridSpec(
            num_scalar_prefetch=1,
            grid=(n_layers, n_slots // TILE),
            in_specs=[
                pl.BlockSpec((TILE, d), only(0)),
                pl.BlockSpec((1, TILE, e), tile),
            ] + [pl.BlockSpec(memory_space=pl.ANY)] * 4,
            out_specs=[
                pl.BlockSpec((1, TILE, d), tile),
                pl.BlockSpec((1, TILE, e), tile),
                pl.BlockSpec((1, TILE, e), tile),
                pl.BlockSpec((1, TILE, ffn), tile),
                pl.BlockSpec((TILE, d), only(n_layers - 1)),
            ],
            scratch_shapes=[
                pltpu.VMEM((n_slots, d), BF16),
                pltpu.VMEM((TILE, d), F32),
            ] + weight_scratch(d, ffn, e),
        ),
        out_shape=[
            jax.ShapeDtypeStruct((n_layers, n_slots, d), BF16),
            jax.ShapeDtypeStruct((n_layers, n_slots, e), F32),
            jax.ShapeDtypeStruct((n_layers, n_slots, e), F32),
            jax.ShapeDtypeStruct((n_layers, n_slots, ffn), F32),
            jax.ShapeDtypeStruct((n_slots, d), BF16),
        ],
        compiler_params=pltpu.CompilerParams(dimension_semantics=("arbitrary", "arbitrary"), vmem_limit_bytes=66_000_000),
        name="forward",
    )(n_tiles, x0, es, w_up, w_down, w_gate, w_proj)


def bwd_kernel(n_ref, *refs):
    @pl.when(pl.program_id(1) < n_ref[0])
    def _():
        bwd_tile(n_ref[0], *refs)


def bwd_tile(n_tiles, lo_ref, hi_ref, cs_ref, ws_ref, cot_ref, ids_ref, xs_ref, g_ref, ge_ref, ug_ref, w_up, w_down, w_gate, w_proj,
             dt_ref, dx_scr, acc, m_scr, parts_scr, up_buf, down_buf, gate_buf, proj_buf, w_sems, out_sems):
    s = pl.program_id(0)
    i = pl.program_id(1)
    n_layers = pl.num_programs(0)
    l = n_layers - 1 - s
    slot = lax.rem(s, 2)
    rows = pl.ds(pl.multiple_of(i * TILE, TILE), TILE)
    range_rows = dt_ref.shape[1]
    n_blk = acc.shape[0] // BLK
    tail = range_rows - (n_blk - 1) * BLK

    @pl.when(i == 0)
    def _():
        next_weights((w_up, w_down, w_gate, w_proj), (up_buf, down_buf, gate_buf, proj_buf), w_sems, s, n_layers, lambda q: n_layers - 1 - q)

    @pl.when(s == 0)
    def _():
        dx_scr[rows, :] = cot_ref[...]

    dx = dx_scr[rows, :]
    d_mixed = nt(dx, proj_buf[slot]).astype(BF16).astype(F32)
    grad_rows = g_ref[0] * d_mixed
    hi_part = grad_rows.astype(BF16)
    rest = grad_rows - hi_part.astype(F32)
    mid_part = rest.astype(BF16)
    parts_scr[0:TILE, :] = hi_part
    parts_scr[TILE:2 * TILE, :] = mid_part
    parts_scr[2 * TILE:3 * TILE, :] = (rest - mid_part.astype(F32)).astype(BF16)

    @pl.when(l > 0)
    def _():
        d_gate_pre = (ge_ref[0] * d_mixed).astype(BF16)
        d_norm_gate = nt(d_gate_pre, gate_buf[slot]).astype(BF16)
        ffn = up_buf.shape[2]
        for c in range(ffn // FCH):
            cs = slice(c * FCH, (c + 1) * FCH)
            d_hid = nt(dx, down_buf[slot, cs, :]).astype(BF16).astype(F32)
            part = nt((ug_ref[0, :, cs] * d_hid).astype(BF16), up_buf[slot, :, cs])
            if c == 0:
                m_scr[...] = part
            else:
                m_scr[...] += part
        xf = xs_ref[0].astype(F32)
        r = norm_stats(xf)
        d_normed = (m_scr[...].astype(BF16) + d_norm_gate).astype(F32)
        dot_xd = jnp.mean(xf * d_normed, axis=-1, keepdims=True)
        d_x = r * d_normed - xf * (r * r * r * dot_xd)
        dx_scr[rows, :] = (dx.astype(F32) + d_x).astype(BF16)

    def block_copy(b, size):
        at = pl.ds(pl.multiple_of(b * BLK, BLK), size)
        return pltpu.make_async_copy(acc.at[at], dt_ref.at[l, at], out_sems.at[b])

    def each_block(first, last, act):
        def step(b, carry):
            act(block_copy(b, BLK))
            return carry

        lax.fori_loop(first, jnp.minimum(last, n_blk - 1), step, 0)

        @pl.when((first < n_blk) & (last == n_blk))
        def _():
            act(block_copy(n_blk - 1, tail))

    @pl.when((s == 0) & (i == 0))
    def _():
        acc[...] = jnp.zeros_like(acc)

    fresh = ws_ref[i]

    @pl.when(s > 0)
    def _():
        each_block(fresh, ws_ref[i + 1], lambda c: c.wait())

    ids = ids_ref[0]

    def scatter_step(b, carry):
        pos = lax.broadcasted_iota(jnp.int32, (BLK, TILE), 0) + b * BLK
        sel = jnp.where(ids == pos, 1.0, 0.0).astype(BF16)
        part = nn(jnp.concatenate([sel, sel, sel], axis=1), parts_scr[...])
        at = pl.ds(pl.multiple_of(b * BLK, BLK), BLK)

        @pl.when(b >= fresh)
        def _():
            acc[at, :] = part

        @pl.when(b < fresh)
        def _():
            acc[at, :] += part

        return carry

    lax.fori_loop(lo_ref[i], hi_ref[i] + 1, scatter_step, 0)
    each_block(cs_ref[i], cs_ref[i + 1], lambda c: c.start())

    @pl.when((l == 0) & (i == n_tiles - 1))
    def _():
        each_block(0, n_blk, lambda c: c.wait())


def backward(n_tiles, lo, hi, cot, ids_row, xs, g, ge, ug, w_up, w_down, w_gate, w_proj, range_rows):
    n_layers, n_slots, d = xs.shape
    e = g.shape[2]
    ffn = w_up.shape[2]
    top = n_layers - 1
    n_blk = pl.cdiv(range_rows, BLK)
    index = jnp.arange(n_slots // TILE + 1, dtype=jnp.int32)
    copy_start = jnp.where(index == 0, 0, jnp.where(index < n_tiles[0], jnp.append(lo, 0), n_blk)).astype(jnp.int32)
    wait_start = jnp.where(index == 0, 0, jnp.where(index < n_tiles[0], jnp.append(0, hi) + 1, n_blk)).astype(jnp.int32)
    tile = lambda s, i, n, *_: (top - s, jnp.minimum(i, n[0] - 1), 0)
    only = lambda which: (lambda s, i, n, *_: (jnp.where(s == which, jnp.minimum(i, n[0] - 1), 0), 0))
    return pl.pallas_call(
        bwd_kernel,
        grid_spec=pltpu.PrefetchScalarGridSpec(
            num_scalar_prefetch=5,
            grid=(n_layers, n_slots // TILE),
            in_specs=[
                pl.BlockSpec((TILE, d), only(0)),
                pl.BlockSpec((1, 1, TILE), lambda s, i, n, *_: (jnp.minimum(i, n[0] - 1), 0, 0)),
                pl.BlockSpec((1, TILE, d), tile),
                pl.BlockSpec((1, TILE, e), tile),
                pl.BlockSpec((1, TILE, e), tile),
                pl.BlockSpec((1, TILE, ffn), tile),
            ] + [pl.BlockSpec(memory_space=pl.ANY)] * 4,
            out_specs=pl.BlockSpec(memory_space=pl.ANY),
            scratch_shapes=[
                pltpu.VMEM((n_slots, d), BF16),
                pltpu.VMEM((n_blk * BLK, e), F32),
                pltpu.VMEM((TILE, d), F32),
                pltpu.VMEM((3 * TILE, e), BF16),
            ] + weight_scratch(d, ffn, e) + [pltpu.SemaphoreType.DMA((n_blk,))],
        ),
        out_shape=jax.ShapeDtypeStruct((n_layers, range_rows, e), F32),
        compiler_params=pltpu.CompilerParams(dimension_semantics=("arbitrary", "arbitrary"), vmem_limit_bytes=66_000_000),
        name="backward",
    )(n_tiles, lo, hi, copy_start, wait_start, cot, ids_row, xs, g, ge, ug, w_up, w_down, w_gate, w_proj)


def solution(mesh):
    n_dp = mesh.shape['dp']
    n_emb = mesh.shape['emb']
    tok_spec = P(('dp', 'emb'))
    act_spec = P(('dp', 'emb'), None)
    table_spec = P(None, 'emb', None)
    full_spec = P(None, None, None)

    def whole_step(tok_ids, resid_in, cot_out, tables, w_up, w_down, w_gate, w_proj):
        range_rows = tables.shape[1]
        tok_count, _ = resid_in.shape
        cap = 2 * tok_count // n_emb
        send_slots = n_emb * cap
        n_slots = n_dp * send_slots

        owner = tok_ids // range_rows
        local_off = tok_ids - owner * range_rows
        one_hot = (owner[:, None] == jnp.arange(n_emb, dtype=jnp.int32)[None, :]).astype(jnp.int32)
        rank_in = jnp.sum((jnp.cumsum(one_hot, axis=0) - one_hot) * one_hot, axis=1)
        slot_of = owner * cap + rank_in
        match = slot_of[None, :] == jnp.arange(send_slots, dtype=jnp.int32)[:, None]
        slot_ids = jnp.min(jnp.where(match, local_off[None, :], SENT), axis=1)
        sel = match.astype(BF16)

        def exchange(a):
            return lax.all_to_all(jnp.concatenate([a] * n_dp, axis=0), ('dp', 'emb'), 0, 0, tiled=True)

        recv_ids = exchange(slot_ids)
        x_slots = exchange(nn(sel, resid_in).astype(BF16))
        cot_slots = exchange(nn(sel, cot_out).astype(BF16))

        raw_key = recv_ids * n_slots + jnp.arange(n_slots, dtype=jnp.int32)
        key = lax.sort(raw_key)
        slot_sorted = key % n_slots
        ids_sorted = key // n_slots
        count = jnp.sum((recv_ids < range_rows).astype(jnp.int32))
        n_tiles = ((count + TILE - 1) // TILE)[None]
        by_tile = ids_sorted.reshape(n_slots // TILE, TILE)
        lo = by_tile[:, 0]
        hi = jnp.max(jnp.where(by_tile < range_rows, by_tile, 0), axis=1)
        own_key = lax.dynamic_slice(raw_key, (lax.axis_index('dp') * send_slots,), (send_slots,))
        own_pos = jnp.sum((raw_key[None, :] < own_key[:, None]).astype(jnp.int32), axis=1)
        slot_col = slot_sorted[:, None]

        es = gather(n_tiles, lo // GBLK, hi // GBLK, ids_sorted[:, None], tables)
        x0 = permute(n_tiles, slot_col, x_slots)
        xs, g, ge, ug, x_last = forward(n_tiles, x0, es, w_up, w_down, w_gate, w_proj)
        back = lax.all_to_all(jnp.take(x_last, own_pos, axis=0), 'emb', 0, 0, tiled=True)
        cot = permute(n_tiles, slot_col, cot_slots)
        d_tables = backward(n_tiles, lo // BLK, hi // BLK, cot, by_tile[:, None, :], xs, g, ge, ug, w_up, w_down, w_gate, w_proj, range_rows)
        resid_out = jnp.take(back, slot_of, axis=0)
        return resid_out, d_tables

    return jax.shard_map(whole_step, mesh=mesh, in_specs=(tok_spec, act_spec, act_spec, table_spec, full_spec, full_spec, full_spec, full_spec), out_specs=(act_spec, table_spec), check_vma=False)
```

```python
import jax
import jax.numpy as jnp
from jax import lax
from jax.experimental import pallas as pl
from jax.experimental.pallas import tpu as pltpu
from jax.sharding import PartitionSpec as P


NORM_EPS = 1e-6
GELU_C = 0.7978845608028654
GELU_A = 0.044715
TILE = 256
BLK = 256
GBLK = 512
PCH = 2048
SUB = 2
FCH = 768
F32 = jnp.float32
BF16 = jnp.bfloat16
SENT = 8191


def gelu_and_grad(x):
    x2 = x * x
    h = 0.5 + 0.5 * jnp.tanh(x * (GELU_C + (GELU_C * GELU_A) * x2))
    y = x * h
    grad = h + (y - y * h) * (2.0 * GELU_C + (6.0 * GELU_C * GELU_A) * x2)
    return y, grad


def nn(a, b):
    return lax.dot_general(a, b, (((1,), (0,)), ((), ())), preferred_element_type=F32)


def nt(a, b):
    return lax.dot_general(a, b, (((1,), (1,)), ((), ())), preferred_element_type=F32)


def norm_stats(xf):
    return lax.rsqrt(jnp.mean(xf * xf, axis=-1, keepdims=True) + NORM_EPS)


def permute_kernel(n_ref, slot_ref, src_ref, out_ref, acc_ref):
    n_slots = src_ref.shape[0]

    @pl.when(pl.program_id(0) < n_ref[0])
    def _():
        slot = slot_ref[...]
        for c in range(n_slots // PCH):
            cols = lax.broadcasted_iota(jnp.int32, (TILE, PCH), 1) + c * PCH
            sel = jnp.where(slot == cols, 1.0, 0.0).astype(BF16)
            part = nn(sel, src_ref[c * PCH:(c + 1) * PCH, :])
            acc = part if c == 0 else acc_ref[...] + part
            if c == n_slots // PCH - 1:
                out_ref[...] = acc.astype(BF16)
            else:
                acc_ref[...] = acc


def permute(n_tiles, slot_col, src):
    n_slots, width = src.shape
    tile = lambda i, n: (jnp.minimum(i, n[0] - 1), 0)
    return pl.pallas_call(
        permute_kernel,
        grid_spec=pltpu.PrefetchScalarGridSpec(
            num_scalar_prefetch=1,
            grid=(n_slots // TILE,),
            in_specs=[
                pl.BlockSpec((TILE, 1), tile),
                pl.BlockSpec((n_slots, width), lambda i, n: (0, 0), pipeline_mode=pl.Buffered(1)),
            ],
            out_specs=pl.BlockSpec((TILE, width), tile),
            scratch_shapes=[pltpu.VMEM((TILE, width), F32)],
        ),
        out_shape=jax.ShapeDtypeStruct((n_slots, width), BF16),
        compiler_params=pltpu.CompilerParams(dimension_semantics=("arbitrary",)),
        name="permute",
    )(n_tiles, slot_col, src)


def gather_kernel(n_ref, lo_ref, hi_ref, ids_ref, table_ref, out_ref, acc_ref):
    range_rows = table_ref.shape[1]

    def tile_step(i, carry):
        rows = pl.ds(pl.multiple_of(i * TILE, TILE), TILE)
        ids = ids_ref[rows, :]

        def part(b):
            start = pl.multiple_of(jnp.minimum(b * GBLK, range_rows - GBLK), 16)
            cols = lax.broadcasted_iota(jnp.int32, (TILE, GBLK), 1) + start
            sel = jnp.where((ids == cols) & (cols >= b * GBLK), 1.0, 0.0).astype(BF16)
            return nn(sel, table_ref[0, pl.ds(start, GBLK), :])

        acc_ref[...] = part(lo_ref[i])

        def step(b, c):
            acc_ref[...] += part(b)
            return c

        lax.fori_loop(lo_ref[i] + 1, hi_ref[i] + 1, step, 0)
        out_ref[0, rows, :] = acc_ref[...].astype(BF16)
        return carry

    lax.fori_loop(0, n_ref[0], tile_step, 0)


def gather(n_tiles, lo, hi, ids_col, tables):
    n_layers, range_rows, e = tables.shape
    n_slots = ids_col.shape[0]
    return pl.pallas_call(
        gather_kernel,
        grid_spec=pltpu.PrefetchScalarGridSpec(
            num_scalar_prefetch=3,
            grid=(n_layers,),
            in_specs=[
                pl.BlockSpec((n_slots, 1), lambda l, *_: (0, 0)),
                pl.BlockSpec((1, range_rows, e), lambda l, *_: (l, 0, 0)),
            ],
            out_specs=pl.BlockSpec((1, n_slots, e), lambda l, *_: (l, 0, 0)),
            scratch_shapes=[pltpu.VMEM((TILE, e), F32)],
        ),
        out_shape=jax.ShapeDtypeStruct((n_layers, n_slots, e), BF16),
        compiler_params=pltpu.CompilerParams(dimension_semantics=("arbitrary",)),
        cost_estimate=pl.CostEstimate(flops=60_000_000_000, bytes_accessed=80_000_000, transcendentals=0),
        name="gather",
    )(n_tiles, lo, hi, ids_col, tables)


def weight_copies(hbm, bufs, sems, layer, slot):
    return [pltpu.make_async_copy(h.at[layer], v.at[slot], sems.at[slot, k]) for k, (h, v) in enumerate(zip(hbm, bufs))]


def next_weights(hbm, bufs, sems, step, n_steps, layer_of):
    slot = lax.rem(step, 2)

    @pl.when(step == 0)
    def _():
        for c in weight_copies(hbm, bufs, sems, layer_of(step), slot):
            c.start()

    for c in weight_copies(hbm, bufs, sems, layer_of(step), slot):
        c.wait()

    @pl.when(step + 1 < n_steps)
    def _():
        for c in weight_copies(hbm, bufs, sems, layer_of(step + 1), 1 - slot):
            c.start()


def weight_scratch(d, ffn, e):
    return [
        pltpu.VMEM((2, d, ffn), BF16),
        pltpu.VMEM((2, ffn, d), BF16),
        pltpu.VMEM((2, d, e), BF16),
        pltpu.VMEM((2, e, d), BF16),
        pltpu.SemaphoreType.DMA((2, 4)),
    ]


def fwd_kernel(n_ref, x0_ref, e_ref, w_up, w_down, w_gate, w_proj, xs_ref, g_ref, ge_ref, ug_ref, xl_ref,
               x_scr, m_scr, up_buf, down_buf, gate_buf, proj_buf, w_sems):
    l = pl.program_id(0)
    i = pl.program_id(1)
    n_layers = pl.num_programs(0)
    slot = lax.rem(l, 2)

    @pl.when(i == 0)
    def _():
        next_weights((w_up, w_down, w_gate, w_proj), (up_buf, down_buf, gate_buf, proj_buf), w_sems, l, n_layers, lambda q: q)

    def sub_tile(h, carry):
        here = pl.ds(pl.multiple_of(h * TILE, TILE), TILE)
        rows = pl.ds(pl.multiple_of((i * SUB + h) * TILE, TILE), TILE)

        @pl.when(l == 0)
        def _():
            x_scr[rows, :] = x0_ref[here, :]

        x = x_scr[rows, :]
        xs_ref[0, here, :] = x
        xf = x.astype(F32)
        u = (xf * norm_stats(xf)).astype(BF16)
        gate, gate_grad = gelu_and_grad(nn(u, gate_buf[slot]))
        emb = e_ref[0, here, :].astype(F32)
        g_ref[0, here, :] = gate
        ge_ref[0, here, :] = gate_grad * emb
        m_scr[...] = xf + nn((gate * emb).astype(BF16), proj_buf[slot])
        ffn = up_buf.shape[2]
        for c in range(ffn // FCH):
            cs = slice(c * FCH, (c + 1) * FCH)
            hid, hid_grad = gelu_and_grad(nn(u, up_buf[slot, :, cs]))
            ug_ref[0, here, cs] = hid_grad
            m_scr[...] += nn(hid.astype(BF16), down_buf[slot, cs, :])
        x_next = m_scr[...].astype(BF16)
        x_scr[rows, :] = x_next

        @pl.when(l == n_layers - 1)
        def _():
            xl_ref[here, :] = x_next

        return carry

    lax.fori_loop(0, jnp.clip(n_ref[0] - i * SUB, 0, SUB), sub_tile, 0)


def forward(n_tiles, x0, es, w_up, w_down, w_gate, w_proj):
    n_layers, n_slots, e = es.shape
    d = x0.shape[1]
    ffn = w_up.shape[2]
    step = SUB * TILE
    last = lambda i, n: jnp.minimum(i, (n[0] + SUB - 1) // SUB - 1)
    tile = lambda l, i, n: (l, last(i, n), 0)
    only = lambda which: (lambda l, i, n: (jnp.where(l == which, last(i, n), 0), 0))
    return pl.pallas_call(
        fwd_kernel,
        grid_spec=pltpu.PrefetchScalarGridSpec(
            num_scalar_prefetch=1,
            grid=(n_layers, n_slots // step),
            in_specs=[
                pl.BlockSpec((step, d), only(0)),
                pl.BlockSpec((1, step, e), tile),
            ] + [pl.BlockSpec(memory_space=pl.ANY)] * 4,
            out_specs=[
                pl.BlockSpec((1, step, d), tile),
                pl.BlockSpec((1, step, e), tile),
                pl.BlockSpec((1, step, e), tile),
                pl.BlockSpec((1, step, ffn), tile),
                pl.BlockSpec((step, d), only(n_layers - 1)),
            ],
            scratch_shapes=[
                pltpu.VMEM((n_slots, d), BF16),
                pltpu.VMEM((TILE, d), F32),
            ] + weight_scratch(d, ffn, e),
        ),
        out_shape=[
            jax.ShapeDtypeStruct((n_layers, n_slots, d), BF16),
            jax.ShapeDtypeStruct((n_layers, n_slots, e), F32),
            jax.ShapeDtypeStruct((n_layers, n_slots, e), F32),
            jax.ShapeDtypeStruct((n_layers, n_slots, ffn), F32),
            jax.ShapeDtypeStruct((n_slots, d), BF16),
        ],
        compiler_params=pltpu.CompilerParams(dimension_semantics=("arbitrary", "arbitrary"), vmem_limit_bytes=66_000_000),
        name="forward",
    )(n_tiles, x0, es, w_up, w_down, w_gate, w_proj)


def bwd_kernel(n_ref, *refs):
    @pl.when(pl.program_id(1) < n_ref[0])
    def _():
        bwd_tile(n_ref[0], *refs)


def bwd_tile(n_tiles, lo_ref, hi_ref, cs_ref, ws_ref, cot_ref, ids_ref, xs_ref, g_ref, ge_ref, ug_ref, w_up, w_down, w_gate, w_proj,
             dt_ref, dx_scr, acc, m_scr, parts_scr, up_buf, down_buf, gate_buf, proj_buf, w_sems, out_sems):
    s = pl.program_id(0)
    i = pl.program_id(1)
    n_layers = pl.num_programs(0)
    l = n_layers - 1 - s
    slot = lax.rem(s, 2)
    rows = pl.ds(pl.multiple_of(i * TILE, TILE), TILE)
    range_rows = dt_ref.shape[1]
    n_blk = acc.shape[0] // BLK
    tail = range_rows - (n_blk - 1) * BLK

    @pl.when(i == 0)
    def _():
        next_weights((w_up, w_down, w_gate, w_proj), (up_buf, down_buf, gate_buf, proj_buf), w_sems, s, n_layers, lambda q: n_layers - 1 - q)

    @pl.when(s == 0)
    def _():
        dx_scr[rows, :] = cot_ref[...]

    dx = dx_scr[rows, :]
    d_mixed = nt(dx, proj_buf[slot]).astype(BF16).astype(F32)
    grad_rows = g_ref[0] * d_mixed
    hi_part = grad_rows.astype(BF16)
    rest = grad_rows - hi_part.astype(F32)
    mid_part = rest.astype(BF16)
    parts_scr[0:TILE, :] = hi_part
    parts_scr[TILE:2 * TILE, :] = mid_part
    parts_scr[2 * TILE:3 * TILE, :] = (rest - mid_part.astype(F32)).astype(BF16)

    @pl.when(l > 0)
    def _():
        d_gate_pre = (ge_ref[0] * d_mixed).astype(BF16)
        d_norm_gate = nt(d_gate_pre, gate_buf[slot]).astype(BF16)
        ffn = up_buf.shape[2]
        for c in range(ffn // FCH):
            cs = slice(c * FCH, (c + 1) * FCH)
            d_hid = nt(dx, down_buf[slot, cs, :]).astype(BF16).astype(F32)
            part = nt((ug_ref[0, :, cs] * d_hid).astype(BF16), up_buf[slot, :, cs])
            if c == 0:
                m_scr[...] = part
            else:
                m_scr[...] += part
        xf = xs_ref[0].astype(F32)
        r = norm_stats(xf)
        d_normed = (m_scr[...].astype(BF16) + d_norm_gate).astype(F32)
        dot_xd = jnp.mean(xf * d_normed, axis=-1, keepdims=True)
        d_x = r * d_normed - xf * (r * r * r * dot_xd)
        dx_scr[rows, :] = (dx.astype(F32) + d_x).astype(BF16)

    def block_copy(b, size):
        at = pl.ds(pl.multiple_of(b * BLK, BLK), size)
        return pltpu.make_async_copy(acc.at[at], dt_ref.at[l, at], out_sems.at[b])

    def each_block(first, last, act):
        def step(b, carry):
            act(block_copy(b, BLK))
            return carry

        lax.fori_loop(first, jnp.minimum(last, n_blk - 1), step, 0)

        @pl.when((first < n_blk) & (last == n_blk))
        def _():
            act(block_copy(n_blk - 1, tail))

    @pl.when((s == 0) & (i == 0))
    def _():
        acc[...] = jnp.zeros_like(acc)

    fresh = ws_ref[i]

    @pl.when(s > 0)
    def _():
        each_block(fresh, ws_ref[i + 1], lambda c: c.wait())

    ids = ids_ref[0]

    def sums(b, blocks):
        pos = lax.broadcasted_iota(jnp.int32, (blocks * BLK, TILE), 0) + b * BLK
        sel = jnp.where(ids == pos, 1.0, 0.0).astype(BF16)
        return nn(jnp.concatenate([sel, sel, sel], axis=1), parts_scr[...])

    def at(b, blocks):
        return pl.ds(pl.multiple_of(b * BLK, BLK), blocks * BLK)

    first = lo_ref[i]
    more = hi_ref[i] - first
    head = sums(first, 1)

    @pl.when(first >= fresh)
    def _():
        acc[at(first, 1), :] = head

    @pl.when(first < fresh)
    def _():
        acc[at(first, 1), :] += head

    def two_blocks(k, carry):
        b = first + 1 + 2 * k
        acc[at(b, 2), :] = sums(b, 2)
        return carry

    lax.fori_loop(0, more // 2, two_blocks, 0)

    @pl.when(lax.rem(more, 2) == 1)
    def _():
        acc[at(first + more, 1), :] = sums(first + more, 1)

    each_block(cs_ref[i], cs_ref[i + 1], lambda c: c.start())

    @pl.when((l == 0) & (i == n_tiles - 1))
    def _():
        each_block(0, n_blk, lambda c: c.wait())


def backward(n_tiles, lo, hi, cot, ids_row, xs, g, ge, ug, w_up, w_down, w_gate, w_proj, range_rows):
    n_layers, n_slots, d = xs.shape
    e = g.shape[2]
    ffn = w_up.shape[2]
    top = n_layers - 1
    n_blk = pl.cdiv(range_rows, BLK)
    index = jnp.arange(n_slots // TILE + 1, dtype=jnp.int32)
    copy_start = jnp.where(index == 0, 0, jnp.where(index < n_tiles[0], jnp.append(lo, 0), n_blk)).astype(jnp.int32)
    wait_start = jnp.where(index == 0, 0, jnp.where(index < n_tiles[0], jnp.append(0, hi) + 1, n_blk)).astype(jnp.int32)
    tile = lambda s, i, n, *_: (top - s, jnp.minimum(i, n[0] - 1), 0)
    only = lambda which: (lambda s, i, n, *_: (jnp.where(s == which, jnp.minimum(i, n[0] - 1), 0), 0))
    return pl.pallas_call(
        bwd_kernel,
        grid_spec=pltpu.PrefetchScalarGridSpec(
            num_scalar_prefetch=5,
            grid=(n_layers, n_slots // TILE),
            in_specs=[
                pl.BlockSpec((TILE, d), only(0)),
                pl.BlockSpec((1, 1, TILE), lambda s, i, n, *_: (jnp.minimum(i, n[0] - 1), 0, 0)),
                pl.BlockSpec((1, TILE, d), tile),
                pl.BlockSpec((1, TILE, e), tile),
                pl.BlockSpec((1, TILE, e), tile),
                pl.BlockSpec((1, TILE, ffn), tile),
            ] + [pl.BlockSpec(memory_space=pl.ANY)] * 4,
            out_specs=pl.BlockSpec(memory_space=pl.ANY),
            scratch_shapes=[
                pltpu.VMEM((n_slots, d), BF16),
                pltpu.VMEM((n_blk * BLK, e), F32),
                pltpu.VMEM((TILE, d), F32),
                pltpu.VMEM((3 * TILE, e), BF16),
            ] + weight_scratch(d, ffn, e) + [pltpu.SemaphoreType.DMA((n_blk,))],
        ),
        out_shape=jax.ShapeDtypeStruct((n_layers, range_rows, e), F32),
        compiler_params=pltpu.CompilerParams(dimension_semantics=("arbitrary", "arbitrary"), vmem_limit_bytes=66_000_000),
        name="backward",
    )(n_tiles, lo, hi, copy_start, wait_start, cot, ids_row, xs, g, ge, ug, w_up, w_down, w_gate, w_proj)


def solution(mesh):
    n_dp = mesh.shape['dp']
    n_emb = mesh.shape['emb']
    tok_spec = P(('dp', 'emb'))
    act_spec = P(('dp', 'emb'), None)
    table_spec = P(None, 'emb', None)
    full_spec = P(None, None, None)

    def whole_step(tok_ids, resid_in, cot_out, tables, w_up, w_down, w_gate, w_proj):
        range_rows = tables.shape[1]
        tok_count, _ = resid_in.shape
        cap = 2 * tok_count // n_emb
        send_slots = n_emb * cap
        n_slots = n_dp * send_slots

        owner = tok_ids // range_rows
        local_off = tok_ids - owner * range_rows
        one_hot = (owner[:, None] == jnp.arange(n_emb, dtype=jnp.int32)[None, :]).astype(jnp.int32)
        rank_in = jnp.sum((jnp.cumsum(one_hot, axis=0) - one_hot) * one_hot, axis=1)
        slot_of = owner * cap + rank_in
        match = slot_of[None, :] == jnp.arange(send_slots, dtype=jnp.int32)[:, None]
        slot_ids = jnp.min(jnp.where(match, local_off[None, :], SENT), axis=1)
        sel = match.astype(BF16)

        def exchange(a):
            return lax.all_to_all(jnp.concatenate([a] * n_dp, axis=0), ('dp', 'emb'), 0, 0, tiled=True)

        recv_ids = exchange(slot_ids)
        x_slots = exchange(nn(sel, resid_in).astype(BF16))
        cot_send = nn(sel, cot_out).astype(BF16)
        cot_slots = exchange(cot_send)

        raw_key = recv_ids * n_slots + jnp.arange(n_slots, dtype=jnp.int32)
        key = lax.sort(raw_key)
        slot_sorted = key % n_slots
        ids_sorted = key // n_slots
        count = jnp.sum((recv_ids < range_rows).astype(jnp.int32))
        n_tiles = ((count + TILE - 1) // TILE)[None]
        by_tile = ids_sorted.reshape(n_slots // TILE, TILE)
        lo = by_tile[:, 0]
        hi = jnp.max(jnp.where(by_tile < range_rows, by_tile, 0), axis=1)
        own_key = lax.dynamic_slice(raw_key, (lax.axis_index('dp') * send_slots,), (send_slots,))
        own_pos = jnp.sum((raw_key[None, :] < own_key[:, None]).astype(jnp.int32), axis=1)
        slot_col = slot_sorted[:, None]

        es = gather(n_tiles, lo // GBLK, hi // GBLK, ids_sorted[:, None], tables)
        x0 = permute(n_tiles, slot_col, x_slots)
        xs, g, ge, ug, x_last = forward(n_tiles, x0, es, w_up, w_down, w_gate, w_proj)
        back = lax.all_to_all(x_last.at[own_pos].get(mode="promise_in_bounds"), 'emb', 0, 0, tiled=True)
        cot = permute(n_tiles, slot_col, cot_slots)
        d_tables = backward(n_tiles, lo // BLK, hi // BLK, cot, by_tile[:, None, :], xs, g, ge, ug, w_up, w_down, w_gate, w_proj, range_rows)
        resid_out = back.at[slot_of].get(mode="promise_in_bounds")
        return resid_out, d_tables

    return jax.shard_map(whole_step, mesh=mesh, in_specs=(tok_spec, act_spec, act_spec, table_spec, full_spec, full_spec, full_spec, full_spec), out_specs=(act_spec, table_spec), check_vma=False)
```
